32 devices in a mesh: batch: 1 (over z), row: 4 (over y), col: 8 (over x, core).
Axes of the slice: x: 4, y: 4, z: 1, core: 2. Of those that a mesh axis runs over, the one named last changes fastest.
The devices are a block of a 4x4x8 slice.
Arguments:
- l_mat: bfloat16 [2048, 2048], P(('batch', 'row'), 'col')
- b_mat: bfloat16 [2048, 65536], P(('batch', 'row'), 'col')
Outputs:
- output: bfloat16 [2048, 65536], P(('batch', 'row'), 'col')
All inputs are finite; a program needn't handle non-finite values.
Results may differ from the reference program's by a relative error of at most 0.001.
Values are sent between devices in bfloat16 or wider.
A program may use at most 768 MiB of HBM per device.

```python
import jax
import jax.numpy as jnp

N = 2048
M = 65536


def setup_inputs(seed: int = 0, part: int = 0) -> dict:
    base_key = jax.random.fold_in(jax.random.key(seed), part)
    key_l, key_b = jax.random.split(base_key)
    row_scale = 1.0 / jnp.sqrt(jnp.arange(N, dtype=jnp.float32) + 1.0)
    l_full = jax.random.normal(key_l, (N, N), jnp.float32)
    l_mat = jnp.tril(l_full) * row_scale[:, None]
    b_mat = jax.random.normal(key_b, (N, M), jnp.float32)
    return {'l_mat': l_mat.astype(jnp.bfloat16), 'b_mat': b_mat.astype(jnp.bfloat16)}


def reference(l_mat, b_mat):
    product = jnp.dot(l_mat, b_mat, preferred_element_type=jnp.float32)
    return product.astype(jnp.bfloat16)
```

```python
import functools

import jax
import jax.numpy as jnp
from jax import lax
from jax.experimental import pallas as pl
from jax.experimental.pallas import tpu as pltpu
from jax.sharding import PartitionSpec as P

MESH = pl.DeviceIdType.MESH
CHUNK = 256
LEAD = 3


def _body(n_row, n_col, l_ref, b_ref, x_ref, lbuf, bbuf, xst,
          l_recv, l_send, l_loc, b_recv, b_loc, send, x_recv, x_loc):
    row = lax.axis_index("row")
    col = lax.axis_index("col")
    m, n = b_ref.shape
    strip = l_ref.shape[1]
    per_block = m // strip
    n_ch = n // CHUNK
    half = n_ch // 2

    barrier = pltpu.get_barrier_semaphore()
    for d in range(1, n_col):
        pl.semaphore_signal(barrier, inc=1, device_id={"col": lax.rem(col + d, n_col)}, device_id_type=MESH)
    for d in (1, n_row - 1):
        pl.semaphore_signal(barrier, inc=1, device_id={"row": lax.rem(row + d, n_row)}, device_id_type=MESH)

    def cols(ch):
        return pl.ds(pl.multiple_of(ch * CHUNK, CHUNK), CHUNK)

    def strip_cols(j):
        return pl.ds(pl.multiple_of(j * strip, strip), strip)

    def block(q, ch):
        return bbuf.at[ch, pl.ds(q * m, m), :]

    def b_load(q, ch):
        return pltpu.make_async_copy(b_ref.at[:, cols(ch)], block(q, ch), b_loc.at[ch])

    def b_own(q, ch, to, kind):
        return pltpu.make_async_remote_copy(
            src_ref=b_ref.at[:, cols(ch)], dst_ref=block(q, ch), send_sem=send.at[kind, ch],
            recv_sem=b_recv.at[q, ch], device_id={"row": to}, device_id_type=MESH)

    def b_fwd(q, ch, to, kind):
        return pltpu.make_async_remote_copy(
            src_ref=block(q, ch), dst_ref=block(q, ch), send_sem=send.at[kind, ch],
            recv_sem=b_recv.at[q, ch], device_id={"row": to}, device_id_type=MESH)

    def x_back(slot, ch, to):
        return pltpu.make_async_remote_copy(
            src_ref=xst.at[slot], dst_ref=x_ref.at[:, cols(ch)], send_sem=send.at[1, ch],
            recv_sem=x_recv.at[lax.rem(ch, half)], device_id={"row": to}, device_id_type=MESH)

    def x_put(slot, ch):
        return pltpu.make_async_copy(xst.at[slot], x_ref.at[:, cols(ch)], x_loc.at[ch])

    def l_place(s, j):
        return lbuf.at[s, :, strip_cols(j)]

    def l_own(s, d):
        return pltpu.make_async_remote_copy(
            src_ref=l_ref, dst_ref=l_place(s, col), send_sem=l_send.at[0, d],
            recv_sem=l_recv.at[s, col], device_id={"col": lax.rem(col + d, n_col)}, device_id_type=MESH)

    def l_fwd(s, d):
        return pltpu.make_async_remote_copy(
            src_ref=l_place(s, col), dst_ref=l_place(s, col), send_sem=l_send.at[1, d],
            recv_sem=l_recv.at[s, col], device_id={"col": lax.rem(col + d, n_col)}, device_id_type=MESH)

    def l_cross(s, to):
        return pltpu.make_async_remote_copy(
            src_ref=l_ref, dst_ref=l_place(s, col), send_sem=l_send.at[0, 0],
            recv_sem=l_recv.at[s, col], device_id={"row": to}, device_id_type=MESH)

    def l_arrival(s, j):
        return pltpu.make_async_remote_copy(
            src_ref=l_ref, dst_ref=l_place(s, j), send_sem=l_send.at[0, 0],
            recv_sem=l_recv.at[s, j], device_id={"col": lax.rem(col + 1, n_col)}, device_id_type=MESH)

    def l_load(s):
        return pltpu.make_async_copy(l_ref, l_place(s, col), l_loc)

    def each(lo, hi, fn):
        def step(i, carry):
            fn(i)
            return carry
        lax.fori_loop(lo, hi, step, 0)

    def dot(s, depth, ch):
        return jnp.dot(lbuf[s, :, :depth], bbuf[ch, :depth, :], preferred_element_type=jnp.float32).astype(xst.dtype)

    def load_start(q, lo, hi):
        each(lo, hi, lambda ch: b_load(q, ch).start())

    def l_gather_start(s, blocks):
        l_load(s).start()

        @pl.when(col < blocks * per_block)
        def _():
            for d in range(1, n_col):
                l_own(s, d).start()

    def l_gather_wait_own(s, blocks):
        for j in range(blocks * per_block):
            @pl.when(col != j)
            def _():
                l_arrival(s, j).wait_recv()

    def l_gather_drain(s, blocks):
        @pl.when(col < blocks * per_block)
        def _():
            for d in range(1, n_col):
                l_own(s, d).wait_send()


    def row0():
        load_start(0, 0, n_ch)
        pl.semaphore_wait(barrier, n_col + 1)
        for i in range(LEAD):
            b_own(0, i, 1, 0).start()
        for i in range(2):
            b_own(0, half + i, 3, 1).start()
        l_gather_start(0, 1)
        l_load(0).wait()
        l_gather_wait_own(0, 1)

        def step(k):
            b_own(0, half + k, 1, 0).start()

            @pl.when(k + LEAD < half)
            def _():
                b_own(0, k + LEAD, 1, 0).start()

            @pl.when(k + 2 < half)
            def _():
                b_own(0, half + k + 2, 3, 1).start()
            b_fwd(1, half + k, 3, 2).wait_recv()
            b_fwd(1, half + k, 3, 2).start()
            for i in range(2):
                ch = 2 * k + i
                b_load(0, ch).wait()
                xst[ch] = dot(0, m, ch)
                x_put(ch, ch).start()
        each(0, half, step)

        def drain(k):
            b_own(0, k, 1, 0).wait_send()
            b_own(0, half + k, 1, 0).wait_send()
            b_own(0, half + k, 3, 1).wait_send()
            b_fwd(1, half + k, 3, 2).wait_send()
            x_put(k, k).wait()
            x_put(half + k, half + k).wait()
        each(0, half, drain)
        l_gather_drain(0, 1)

    def row1():
        load_start(1, 0, n_ch)
        pl.semaphore_wait(barrier, n_col + 1)
        for i in range(LEAD):
            b_own(1, i, 2, 0).start()
            b_own(1, half + i, 0, 2).start()
        l_gather_start(0, 2)
        l_load(0).wait()
        l_gather_wait_own(0, 2)

        def product(ch):
            b_load(1, ch).wait()
            xst[ch] = dot(0, 2 * m, ch)
            x_put(ch, ch).start()

        def step(k):
            b_fwd(0, k, 2, 1).wait_recv()
            b_fwd(0, k, 2, 1).start()

            @pl.when(k + LEAD < half)
            def _():
                b_own(1, k + LEAD, 2, 0).start()
                b_own(1, half + k + LEAD, 0, 2).start()
            product(k)

            @pl.when(k >= LEAD)
            def _():
                b_fwd(0, half + k - LEAD, 2, 1).wait_recv()
                product(half + k - LEAD)
        each(0, half, step)

        def tail(k):
            b_fwd(0, k, 2, 1).wait_recv()
            product(k)
        each(n_ch - LEAD, n_ch, tail)

        def drain(k):
            b_own(1, k, 2, 0).wait_send()
            b_own(1, half + k, 0, 2).wait_send()
            b_fwd(0, k, 2, 1).wait_send()
            x_put(k, k).wait()
            x_put(half + k, half + k).wait()
        each(0, half, drain)
        l_gather_drain(0, 2)

    def lower(p):
        o = 5 - p
        s, so = p - 2, o - 2
        base, other = s * half, so * half
        load_start(p, base, base + half)
        pl.semaphore_wait(barrier, n_col + 1)

        @pl.when(col < (p + 1) * per_block)
        def _():
            l_cross(s, o).start()
        l_gather_start(s, p + 1)
        each(other, other + half, lambda ch: b_own(p, ch, o, 0).start())

        @pl.when(col < (o + 1) * per_block)
        def _():
            l_arrival(so, col).wait_recv()
            for d in range(1, n_col):
                l_fwd(so, d).start()
        l_load(s).wait()
        l_gather_wait_own(s, p + 1)
        l_gather_wait_own(so, o + 1)

        def step(ch):
            for q in range(4):
                if q != p:
                    b_fwd(q, ch, o, 0).wait_recv()
            b_load(p, ch).wait()
            away = 2 * (ch - base)
            xst[away] = dot(so, (o + 1) * m, ch)
            x_back(away, ch, o).start()
            xst[away + 1] = dot(s, (p + 1) * m, ch)
            x_put(away + 1, ch).start()
        each(base, base + half, step)

        def drain(k):
            b_own(p, other + k, o, 0).wait_send()
            x_back(2 * k, base + k, o).wait_send()
            x_put(2 * k + 1, base + k).wait()
            x_back(2 * k, other + k, o).wait_recv()
        each(0, half, drain)
        l_gather_drain(s, p + 1)

        @pl.when(col < (p + 1) * per_block)
        def _():
            l_cross(s, o).wait_send()

        @pl.when(col < (o + 1) * per_block)
        def _():
            for d in range(1, n_col):
                l_fwd(so, d).wait_send()

    pl.when(row == 0)(row0)
    pl.when(row == 1)(row1)
    pl.when(row == 2)(functools.partial(lower, 2))
    pl.when(row == 3)(functools.partial(lower, 3))


def solution(mesh):
    spec = P(("batch", "row"), "col")
    n_row, n_col = mesh.shape["row"], mesh.shape["col"]
    assert n_row == 4

    def local(l_block, b_block):
        m, n = b_block.shape
        k = n_row * m
        n_ch = n // CHUNK
        dma = pltpu.SemaphoreType.DMA
        return pl.pallas_call(
            functools.partial(_body, n_row, n_col),
            out_shape=jax.ShapeDtypeStruct((m, n), b_block.dtype),
            in_specs=[pl.BlockSpec(memory_space=pl.ANY)] * 2,
            out_specs=pl.BlockSpec(memory_space=pl.ANY),
            scratch_shapes=[
                pltpu.VMEM((2, m, k), l_block.dtype),
                pltpu.VMEM((n_ch, k, CHUNK), b_block.dtype),
                pltpu.VMEM((n_ch, m, CHUNK), b_block.dtype),
                dma((2, n_col)),
                dma((2, n_col)),
                dma(()),
                dma((n_row, n_ch)),
                dma((n_ch,)),
                dma((3, n_ch)),
                dma((n_ch // 2,)),
                dma((n_ch,)),
            ],
            compiler_params=pltpu.CompilerParams(
                collective_id=0, has_side_effects=True, vmem_limit_bytes=60 * 1024 * 1024),
            name="tri_ring",
        )(l_block, b_block)

    return jax.shard_map(local, mesh=mesh, in_specs=(spec, spec), out_specs=spec, check_vma=False)
```

```python
import functools

import jax
import jax.numpy as jnp
from jax import lax
from jax.experimental import pallas as pl
from jax.experimental.pallas import tpu as pltpu
from jax.sharding import PartitionSpec as P

MESH = pl.DeviceIdType.MESH
CHUNK = 256
LEAD = 3
LAG = 4
STORES = 8


def _body(n_row, n_col, l_ref, b_ref, x_ref, lbuf, bbuf, xst,
          l_recv, l_send, l_loc, b_recv, b_loc, send, x_recv):
    row = lax.axis_index("row")
    col = lax.axis_index("col")
    m, n = b_ref.shape
    strip = l_ref.shape[1]
    per_block = m // strip
    n_ch = n // CHUNK
    half = n_ch // 2

    barrier = pltpu.get_barrier_semaphore()
    for d in range(1, n_col):
        pl.semaphore_signal(barrier, inc=1, device_id={"col": lax.rem(col + d, n_col)}, device_id_type=MESH)
    for d in (1, n_row - 1):
        pl.semaphore_signal(barrier, inc=1, device_id={"row": lax.rem(row + d, n_row)}, device_id_type=MESH)

    def cols(ch):
        return pl.ds(pl.multiple_of(ch * CHUNK, CHUNK), CHUNK)

    def strip_cols(j):
        return pl.ds(pl.multiple_of(j * strip, strip), strip)

    def block(q, ch):
        return bbuf.at[ch, pl.ds(q * m, m), :]

    def b_load(q, ch):
        return pltpu.make_async_copy(b_ref.at[:, cols(ch)], block(q, ch), b_loc.at[ch])

    def b_own(q, ch, to, kind):
        return pltpu.make_async_remote_copy(
            src_ref=b_ref.at[:, cols(ch)], dst_ref=block(q, ch), send_sem=send.at[kind, ch],
            recv_sem=b_recv.at[q, ch], device_id={"row": to}, device_id_type=MESH)

    def b_fwd(q, ch, to, kind):
        return pltpu.make_async_remote_copy(
            src_ref=block(q, ch), dst_ref=block(q, ch), send_sem=send.at[kind, ch],
            recv_sem=b_recv.at[q, ch], device_id={"row": to}, device_id_type=MESH)

    def x_back(slot, ch, to):
        return pltpu.make_async_remote_copy(
            src_ref=xst.at[slot], dst_ref=x_ref.at[:, cols(ch)], send_sem=send.at[1, ch],
            recv_sem=x_recv.at[lax.rem(ch, half)], device_id={"row": to}, device_id_type=MESH)

    def l_place(s, j):
        return lbuf.at[s, :, strip_cols(j)]

    def l_own(s, d):
        return pltpu.make_async_remote_copy(
            src_ref=l_ref, dst_ref=l_place(s, col), send_sem=l_send.at[0, d],
            recv_sem=l_recv.at[s, col], device_id={"col": lax.rem(col + d, n_col)}, device_id_type=MESH)

    def l_fwd(s, d):
        return pltpu.make_async_remote_copy(
            src_ref=l_place(s, col), dst_ref=l_place(s, col), send_sem=l_send.at[1, d],
            recv_sem=l_recv.at[s, col], device_id={"col": lax.rem(col + d, n_col)}, device_id_type=MESH)

    def l_cross(s, to):
        return pltpu.make_async_remote_copy(
            src_ref=l_ref, dst_ref=l_place(s, col), send_sem=l_send.at[0, 0],
            recv_sem=l_recv.at[s, col], device_id={"row": to}, device_id_type=MESH)

    def l_arrival(s, j):
        return pltpu.make_async_remote_copy(
            src_ref=l_ref, dst_ref=l_place(s, j), send_sem=l_send.at[0, 0],
            recv_sem=l_recv.at[s, j], device_id={"col": lax.rem(col + 1, n_col)}, device_id_type=MESH)

    def l_load(s):
        return pltpu.make_async_copy(l_ref, l_place(s, col), l_loc)

    def each(lo, hi, fn):
        def step(i, carry):
            fn(i)
            return carry
        lax.fori_loop(lo, hi, step, 0)

    def dot(s, depth, ch):
        return jnp.dot(lbuf[s, :, :depth], bbuf[ch, :depth, :], preferred_element_type=jnp.float32).astype(xst.dtype)

    def load_start(q, lo, hi):
        each(lo, hi, lambda ch: b_load(q, ch).start())

    def l_gather_start(s, blocks):
        l_load(s).start()

        @pl.when(col < blocks * per_block)
        def _():
            for d in range(1, n_col):
                l_own(s, d).start()

    def l_gather_wait_own(s, blocks):
        for j in range(blocks * per_block):
            @pl.when(col != j)
            def _():
                l_arrival(s, j).wait_recv()

    def l_gather_drain(s, blocks):
        @pl.when(col < blocks * per_block)
        def _():
            for d in range(1, n_col):
                l_own(s, d).wait_send()


    def row0():
        load_start(0, 0, n_ch)
        pl.semaphore_wait(barrier, n_col + 1)
        for i in range(LEAD):
            b_own(0, i, 1, 0).start()
        for i in range(2):
            b_own(0, half + i, 3, 1).start()
        l_gather_start(0, 1)

        def product(ch):
            b_load(0, ch).wait()
            x_ref[:, cols(ch)] = dot(0, m, ch)

        def step(k):
            b_own(0, half + k, 1, 0).start()

            @pl.when(k + LEAD < half)
            def _():
                b_own(0, k + LEAD, 1, 0).start()

            @pl.when(k + 2 < half)
            def _():
                b_own(0, half + k + 2, 3, 1).start()
            b_fwd(1, half + k, 3, 2).wait_recv()
            b_fwd(1, half + k, 3, 2).start()

            @pl.when(k == LAG)
            def _():
                l_load(0).wait()
                l_gather_wait_own(0, 1)

            @pl.when(k >= LAG)
            def _():
                done = (k - LAG) * n_ch // (half - LAG)
                each(done, (k + 1 - LAG) * n_ch // (half - LAG), product)
        each(0, half, step)

        def drain(k):
            b_own(0, k, 1, 0).wait_send()
            b_own(0, half + k, 1, 0).wait_send()
            b_own(0, half + k, 3, 1).wait_send()
            b_fwd(1, half + k, 3, 2).wait_send()
        each(0, half, drain)
        l_gather_drain(0, 1)

    def row1():
        load_start(1, 0, n_ch)
        pl.semaphore_wait(barrier, n_col + 1)
        for i in range(LEAD):
            b_own(1, i, 2, 0).start()
            b_own(1, half + i, 0, 2).start()
        l_gather_start(0, 2)

        def product(ch):
            b_load(1, ch).wait()
            x_ref[:, cols(ch)] = dot(0, 2 * m, ch)

        def late_product(ch):
            b_fwd(0, ch, 2, 1).wait_recv()
            product(ch)

        def first_done(k):
            return jnp.clip(2 * (k + 1 - LAG), 0, k + 1)

        def second_done(k):
            return jnp.clip(2 * (k + 1 - LAG), 0, jnp.maximum(k + 1 - LEAD, 0))

        def step(k):
            b_fwd(0, k, 2, 1).wait_recv()
            b_fwd(0, k, 2, 1).start()

            @pl.when(k + LEAD < half)
            def _():
                b_own(1, k + LEAD, 2, 0).start()
                b_own(1, half + k + LEAD, 0, 2).start()

            @pl.when(k == LAG)
            def _():
                l_load(0).wait()
                l_gather_wait_own(0, 2)
            each(first_done(k - 1), first_done(k), product)
            each(half + second_done(k - 1), half + second_done(k), late_product)
        each(0, half, step)
        each(n_ch - LEAD, n_ch, late_product)

        def drain(k):
            b_own(1, k, 2, 0).wait_send()
            b_own(1, half + k, 0, 2).wait_send()
            b_fwd(0, k, 2, 1).wait_send()
        each(0, half, drain)
        l_gather_drain(0, 2)

    def lower(p):
        o = 5 - p
        s, so = p - 2, o - 2
        base, other = s * half, so * half
        load_start(p, base, base + half)
        pl.semaphore_wait(barrier, n_col + 1)

        @pl.when(col < (p + 1) * per_block)
        def _():
            l_cross(s, o).start()
        l_gather_start(s, p + 1)
        each(other, other + half, lambda ch: b_own(p, ch, o, 0).start())

        @pl.when(col < (o + 1) * per_block)
        def _():
            l_arrival(so, col).wait_recv()
            for d in range(1, n_col):
                l_fwd(so, d).start()
        l_load(s).wait()
        l_gather_wait_own(s, p + 1)
        l_gather_wait_own(so, o + 1)

        def step(ch):
            for q in range(4):
                if q != p:
                    b_fwd(q, ch, o, 0).wait_recv()
            b_load(p, ch).wait()
            away = ch - base
            xst[away] = dot(so, (o + 1) * m, ch)
            x_back(away, ch, o).start()
            x_ref[:, cols(ch)] = dot(s, (p + 1) * m, ch)
        each(base, base + half, step)

        def drain(k):
            b_own(p, other + k, o, 0).wait_send()
            x_back(k, base + k, o).wait_send()
            x_back(k, other + k, o).wait_recv()
        each(0, half, drain)
        l_gather_drain(s, p + 1)

        @pl.when(col < (p + 1) * per_block)
        def _():
            l_cross(s, o).wait_send()

        @pl.when(col < (o + 1) * per_block)
        def _():
            for d in range(1, n_col):
                l_fwd(so, d).wait_send()

    pl.when(row == 0)(row0)
    pl.when(row == 1)(row1)
    pl.when(row == 2)(functools.partial(lower, 2))
    pl.when(row == 3)(functools.partial(lower, 3))


def _store_body(v_ref, x_ref, sem):
    rows = v_ref.shape[0] // STORES
    copies = [pltpu.make_async_copy(v_ref.at[pl.ds(i * rows, rows), :], x_ref.at[pl.ds(i * rows, rows), :], sem.at[i])
              for i in range(STORES)]
    for copy in copies:
        copy.start()
    for copy in copies:
        copy.wait()


def solution(mesh):
    spec = P(("batch", "row"), "col")
    n_row, n_col = mesh.shape["row"], mesh.shape["col"]
    assert n_row == 4

    def local(l_block, b_block):
        m, n = b_block.shape
        k = n_row * m
        n_ch = n // CHUNK
        dma = pltpu.SemaphoreType.DMA
        x = pl.pallas_call(
            functools.partial(_body, n_row, n_col),
            out_shape=pltpu.VMEM((m, n), b_block.dtype),
            in_specs=[pl.BlockSpec(memory_space=pl.ANY)] * 2,
            out_specs=pl.BlockSpec(memory_space=pltpu.VMEM),
            scratch_shapes=[
                pltpu.VMEM((2, m, k), l_block.dtype),
                pltpu.VMEM((n_ch, k, CHUNK), b_block.dtype),
                pltpu.VMEM((n_ch // 2, m, CHUNK), b_block.dtype),
                dma((2, n_col)),
                dma((2, n_col)),
                dma(()),
                dma((n_row, n_ch)),
                dma((n_ch,)),
                dma((3, n_ch)),
                dma((n_ch // 2,)),
            ],
            compiler_params=pltpu.CompilerParams(
                collective_id=0, has_side_effects=True, vmem_limit_bytes=50 * 1024 * 1024),
            name="tri_ring",
        )(l_block, b_block)
        return pl.pallas_call(
            _store_body,
            out_shape=jax.ShapeDtypeStruct((m, n), b_block.dtype),
            in_specs=[pl.BlockSpec(memory_space=pltpu.VMEM)],
            out_specs=pl.BlockSpec(memory_space=pl.ANY),
            scratch_shapes=[dma((STORES,))],
            compiler_params=pltpu.CompilerParams(vmem_limit_bytes=1024 * 1024),
            name="tri_store",
        )(pltpu.with_memory_space_constraint(x, pltpu.VMEM))

    return jax.shard_map(local, mesh=mesh, in_specs=(spec, spec), out_specs=spec, check_vma=False)
```

```python
import functools

import jax
import jax.numpy as jnp
from jax import lax
from jax.experimental import pallas as pl
from jax.experimental.pallas import tpu as pltpu
from jax.sharding import PartitionSpec as P

MESH = pl.DeviceIdType.MESH
CHUNK = 256
DIRECT = 2
LEAD = 3
LEAD_A = 5
RELAY = 2
LAG = 4
SPECIAL = 9
STORES = 8


def _body(n_row, n_col, l_ref, b_ref, x_ref, lbuf, bbuf, xst,
          l_recv, l_send, l_loc, b_recv, b_loc, send, x_recv):
    row = lax.axis_index("row")
    col = lax.axis_index("col")
    m, n = b_ref.shape
    strip = l_ref.shape[1]
    per_block = m // strip
    n_ch = n // CHUNK
    half = (n_ch - DIRECT) // 2
    top = 2 * half

    barrier = pltpu.get_barrier_semaphore()
    for d in range(1, n_col):
        pl.semaphore_signal(barrier, inc=1, device_id={"col": lax.rem(col + d, n_col)}, device_id_type=MESH)
    for d in (1, n_row - 1):
        pl.semaphore_signal(barrier, inc=1, device_id={"row": lax.rem(row + d, n_row)}, device_id_type=MESH)

    def cols(ch):
        return pl.ds(pl.multiple_of(ch * CHUNK, CHUNK), CHUNK)

    def strip_cols(j):
        return pl.ds(pl.multiple_of(j * strip, strip), strip)

    def block(q, ch):
        return bbuf.at[ch, pl.ds(q * m, m), :]

    def b_load(q, ch):
        return pltpu.make_async_copy(b_ref.at[:, cols(ch)], block(q, ch), b_loc.at[ch])

    def b_own(q, ch, to, kind):
        return pltpu.make_async_remote_copy(
            src_ref=b_ref.at[:, cols(ch)], dst_ref=block(q, ch), send_sem=send.at[kind, ch],
            recv_sem=b_recv.at[q, ch], device_id={"row": to}, device_id_type=MESH)

    def b_fwd(q, ch, to, kind):
        return pltpu.make_async_remote_copy(
            src_ref=block(q, ch), dst_ref=block(q, ch), send_sem=send.at[kind, ch],
            recv_sem=b_recv.at[q, ch], device_id={"row": to}, device_id_type=MESH)

    def x_back(slot, ch, to):
        return pltpu.make_async_remote_copy(
            src_ref=xst.at[slot], dst_ref=x_ref.at[:, cols(ch)], send_sem=send.at[1, ch],
            recv_sem=x_recv.at[ch], device_id={"row": to}, device_id_type=MESH)

    def l_place(s, j):
        return lbuf.at[s, :, strip_cols(j)]

    def l_own(s, d):
        return pltpu.make_async_remote_copy(
            src_ref=l_ref, dst_ref=l_place(s, col), send_sem=l_send.at[0, d],
            recv_sem=l_recv.at[s, col], device_id={"col": lax.rem(col + d, n_col)}, device_id_type=MESH)

    def l_fwd(s, d):
        return pltpu.make_async_remote_copy(
            src_ref=l_place(s, col), dst_ref=l_place(s, col), send_sem=l_send.at[1, d],
            recv_sem=l_recv.at[s, col], device_id={"col": lax.rem(col + d, n_col)}, device_id_type=MESH)

    def l_cross(s, to, kind):
        return pltpu.make_async_remote_copy(
            src_ref=l_ref, dst_ref=l_place(s, col), send_sem=l_send.at[kind, 0],
            recv_sem=l_recv.at[s, col], device_id={"row": to}, device_id_type=MESH)

    def l_arrival(s, j):
        return pltpu.make_async_remote_copy(
            src_ref=l_ref, dst_ref=l_place(s, j), send_sem=l_send.at[0, 0],
            recv_sem=l_recv.at[s, j], device_id={"col": lax.rem(col + 1, n_col)}, device_id_type=MESH)

    def l_load(s):
        return pltpu.make_async_copy(l_ref, l_place(s, col), l_loc)

    def each(lo, hi, fn):
        def step(i, carry):
            fn(i)
            return carry
        lax.fori_loop(lo, hi, step, 0)

    def dot(s, depth, ch):
        return jnp.dot(lbuf[s, :, :depth], bbuf[ch, :depth, :], preferred_element_type=jnp.float32).astype(xst.dtype)

    def load_start(q, lo, hi):
        each(lo, hi, lambda ch: b_load(q, ch).start())


    def holds(blocks):
        return col < blocks * per_block

    def l_gather_start(s, blocks):
        l_load(s).start()

        @pl.when(holds(blocks))
        def _():
            for d in range(1, n_col):
                l_own(s, d).start()

    def l_gather_wait(s, blocks):
        for j in range(blocks * per_block):
            @pl.when(col != j)
            def _():
                l_arrival(s, j).wait_recv()

    def l_gather_drain(s, blocks):
        @pl.when(holds(blocks))
        def _():
            for d in range(1, n_col):
                l_own(s, d).wait_send()

    def l_relay_start(s, blocks):
        @pl.when(holds(blocks))
        def _():
            l_arrival(s, col).wait_recv()
            for d in range(1, n_col):
                l_fwd(s, d).start()

    def l_relay_drain(s, blocks):
        @pl.when(holds(blocks))
        def _():
            for d in range(1, n_col):
                l_fwd(s, d).wait_send()


    def row0():
        load_start(0, 0, n_ch)
        pl.semaphore_wait(barrier, n_col + 1)
        for i in range(LEAD_A):
            b_own(0, i, 1, 0).start()
        for i in range(LEAD):
            b_own(0, half + i, 3, 1).start()
        each(top, n_ch, lambda ch: b_own(0, ch, 1, 0).start())
        l_gather_start(0, 1)

        def product(ch):
            b_load(0, ch).wait()
            x_ref[:, cols(ch)] = dot(0, m, ch)

        def special(ch):
            product(ch)
            for q in range(1, 4):
                b_fwd(q, ch, 1, 0).wait_recv()
            xst[ch - top] = dot(1, 4 * m, ch)

        def step(k):
            b_own(0, half + k, 1, 0).start()

            @pl.when(k + LEAD_A < half)
            def _():
                b_own(0, k + LEAD_A, 1, 0).start()

            @pl.when(k + LEAD < half)
            def _():
                b_own(0, half + k + LEAD, 3, 1).start()
            b_fwd(1, half + k, 3, 2).wait_recv()
            b_fwd(1, half + k, 3, 2).start()

            @pl.when(k == half - 1)
            def _():
                each(top, n_ch, lambda ch: x_back(ch - top, ch, 3).start())

            @pl.when(k == RELAY)
            def _():
                l_relay_start(1, 4)

            @pl.when(k == LAG)
            def _():
                l_load(0).wait()
                l_gather_wait(0, 1)

            @pl.when(k >= LAG)
            def _():
                done = (k - LAG) * top // (half - LAG)
                each(done, (k + 1 - LAG) * top // (half - LAG), product)

            @pl.when(k == SPECIAL)
            def _():
                l_gather_wait(1, 4)
                each(top, n_ch, special)
        each(0, half, step)

        def drain(k):
            b_own(0, k, 1, 0).wait_send()
            b_own(0, half + k, 1, 0).wait_send()
            b_own(0, half + k, 3, 1).wait_send()
            b_fwd(1, half + k, 3, 2).wait_send()
        each(0, half, drain)

        def drain_special(ch):
            b_own(0, ch, 1, 0).wait_send()
            x_back(ch - top, ch, 3).wait_send()
        each(top, n_ch, drain_special)
        l_gather_drain(0, 1)
        l_relay_drain(1, 4)

    def row1():
        load_start(1, 0, n_ch)
        pl.semaphore_wait(barrier, n_col + 1)
        for i in range(LEAD):
            b_own(1, i, 2, 0).start()
            b_own(1, half + i, 0, 2).start()
        l_gather_start(0, 2)

        def product(ch):
            b_load(1, ch).wait()
            x_ref[:, cols(ch)] = dot(0, 2 * m, ch)

        def late_product(ch):
            b_fwd(0, ch, 2, 1).wait_recv()
            product(ch)

        def special(ch):
            late_product(ch)
            xst[ch - top] = dot(1, 3 * m, ch)

        def special_relay(ch):
            b_own(1, ch, 0, 2).start()
            b_fwd(2, ch, 0, 0).wait_recv()
            b_fwd(2, ch, 0, 0).start()

        def first_done(k):
            return jnp.clip(2 * (k + 1 - LAG), 0, k + 1)

        def second_done(k):
            return jnp.clip(2 * (k + 1 - LAG), 0, jnp.maximum(k + 1 - LEAD_A, 0))

        def step(k):
            b_fwd(0, k, 2, 1).wait_recv()
            b_fwd(0, k, 2, 1).start()

            @pl.when(k + LEAD < half)
            def _():
                b_own(1, k + LEAD, 2, 0).start()
                b_own(1, half + k + LEAD, 0, 2).start()

            @pl.when(k == half - 1)
            def _():
                each(top, n_ch, lambda ch: x_back(ch - top, ch, 2).start())

            @pl.when(k == RELAY)
            def _():
                each(top, n_ch, special_relay)
                l_relay_start(1, 3)

            @pl.when(k == LAG)
            def _():
                l_load(0).wait()
                l_gather_wait(0, 2)
            each(first_done(k - 1), first_done(k), product)
            each(half + second_done(k - 1), half + second_done(k), late_product)

            @pl.when(k == SPECIAL)
            def _():
                l_gather_wait(1, 3)
                each(top, n_ch, special)
        each(0, half, step)
        each(top - LEAD_A, top, late_product)

        def drain(k):
            b_own(1, k, 2, 0).wait_send()
            b_own(1, half + k, 0, 2).wait_send()
            b_fwd(0, k, 2, 1).wait_send()
        each(0, half, drain)

        def drain_special(ch):
            b_own(1, ch, 0, 2).wait_send()
            b_fwd(2, ch, 0, 0).wait_send()
            x_back(ch - top, ch, 2).wait_send()
        each(top, n_ch, drain_special)
        l_gather_drain(0, 2)
        l_relay_drain(1, 3)

    def lower(p):
        o, u = 5 - p, 1 if p == 2 else 0
        s, so = p - 2, o - 2
        base, other = s * half, so * half
        load_start(p, base, base + half)
        pl.semaphore_wait(barrier, n_col + 1)

        @pl.when(holds(p + 1))
        def _():
            l_cross(s, o, 0).start()
            l_cross(1, u, 1).start()
        l_gather_start(s, p + 1)
        each(top, n_ch, lambda ch: b_own(p, ch, u, 0).start())
        each(other, other + half, lambda ch: b_own(p, ch, o, 0).start())
        l_relay_start(so, o + 1)
        l_load(s).wait()
        l_gather_wait(s, p + 1)
        l_gather_wait(so, o + 1)

        def step(ch):
            for q in range(4):
                if q != p:
                    b_fwd(q, ch, o, 0).wait_recv()
            b_load(p, ch).wait()
            away = ch - base
            xst[away] = dot(so, (o + 1) * m, ch)
            x_back(away, ch, o).start()
            x_ref[:, cols(ch)] = dot(s, (p + 1) * m, ch)
        each(base, base + half, step)

        def drain(k):
            b_own(p, other + k, o, 0).wait_send()
            x_back(k, base + k, o).wait_send()
            x_back(k, other + k, o).wait_recv()
        each(0, half, drain)

        def drain_special(ch):
            b_own(p, ch, u, 0).wait_send()
            x_back(ch - top, ch, u).wait_recv()
        each(top, n_ch, drain_special)
        l_gather_drain(s, p + 1)
        l_relay_drain(so, o + 1)

        @pl.when(holds(p + 1))
        def _():
            l_cross(s, o, 0).wait_send()
            l_cross(1, u, 1).wait_send()

    pl.when(row == 0)(row0)
    pl.when(row == 1)(row1)
    pl.when(row == 2)(functools.partial(lower, 2))
    pl.when(row == 3)(functools.partial(lower, 3))


def _store_body(v_ref, x_ref, sem):
    rows = v_ref.shape[0] // STORES
    copies = [pltpu.make_async_copy(v_ref.at[pl.ds(i * rows, rows), :], x_ref.at[pl.ds(i * rows, rows), :], sem.at[i])
              for i in range(STORES)]
    for copy in copies:
        copy.start()
    for copy in copies:
        copy.wait()


def solution(mesh):
    spec = P(("batch", "row"), "col")
    n_row, n_col = mesh.shape["row"], mesh.shape["col"]
    assert n_row == 4

    def local(l_block, b_block):
        m, n = b_block.shape
        k = n_row * m
        n_ch = n // CHUNK
        dma = pltpu.SemaphoreType.DMA
        x = pl.pallas_call(
            functools.partial(_body, n_row, n_col),
            out_shape=pltpu.VMEM((m, n), b_block.dtype),
            in_specs=[pl.BlockSpec(memory_space=pl.ANY)] * 2,
            out_specs=pl.BlockSpec(memory_space=pltpu.VMEM),
            scratch_shapes=[
                pltpu.VMEM((2, m, k), l_block.dtype),
                pltpu.VMEM((n_ch, k, CHUNK), b_block.dtype),
                pltpu.VMEM(((n_ch - DIRECT) // 2, m, CHUNK), b_block.dtype),
                dma((2, n_col)),
                dma((2, n_col)),
                dma(()),
                dma((n_row, n_ch)),
                dma((n_ch,)),
                dma((3, n_ch)),
                dma((n_ch,)),
            ],
            compiler_params=pltpu.CompilerParams(
                collective_id=0, has_side_effects=True, vmem_limit_bytes=50 * 1024 * 1024),
            name="tri_ring",
        )(l_block, b_block)
        return pl.pallas_call(
            _store_body,
            out_shape=jax.ShapeDtypeStruct((m, n), b_block.dtype),
            in_specs=[pl.BlockSpec(memory_space=pltpu.VMEM)],
            out_specs=pl.BlockSpec(memory_space=pl.ANY),
            scratch_shapes=[dma((STORES,))],
            compiler_params=pltpu.CompilerParams(vmem_limit_bytes=1024 * 1024),
            name="tri_store",
        )(pltpu.with_memory_space_constraint(x, pltpu.VMEM))

    return jax.shard_map(local, mesh=mesh, in_specs=(spec, spec), out_specs=spec, check_vma=False)
```

```python
import functools

import jax
import jax.numpy as jnp
from jax import lax
from jax.experimental import pallas as pl
from jax.experimental.pallas import tpu as pltpu
from jax.sharding import PartitionSpec as P

MESH = pl.DeviceIdType.MESH
CHUNK = 512
DIRECT = 2
LEAD = 2
LEAD_A = 3
RELAY = 1
LAG = 3
SPECIAL = 5
STORES = 8


def _body(n_row, n_col, l_ref, b_ref, x_ref, lbuf, bbuf, xst,
          l_recv, l_send, l_loc, b_recv, b_loc, send, x_recv):
    row = lax.axis_index("row")
    col = lax.axis_index("col")
    m, n = b_ref.shape
    strip = l_ref.shape[1]
    per_block = m // strip
    n_ch = n // CHUNK
    half = (n_ch - DIRECT) // 2
    top = 2 * half

    barrier = pltpu.get_barrier_semaphore()
    for d in (1, n_row - 1):
        pl.semaphore_signal(barrier, inc=1, device_id={"row": lax.rem(row + d, n_row)}, device_id_type=MESH)
    for d in range(1, n_col):
        pl.semaphore_signal(barrier, inc=1, device_id={"col": lax.rem(col + d, n_col)}, device_id_type=MESH)

    def cols(ch):
        return pl.ds(pl.multiple_of(ch * CHUNK, CHUNK), CHUNK)

    def strip_cols(j):
        return pl.ds(pl.multiple_of(j * strip, strip), strip)

    def block(q, ch):
        return bbuf.at[ch, pl.ds(q * m, m), :]

    def b_load(q, ch):
        return pltpu.make_async_copy(b_ref.at[:, cols(ch)], block(q, ch), b_loc.at[ch])

    def b_own(q, ch, to, kind):
        return pltpu.make_async_remote_copy(
            src_ref=b_ref.at[:, cols(ch)], dst_ref=block(q, ch), send_sem=send.at[kind, ch],
            recv_sem=b_recv.at[q, ch], device_id={"row": to}, device_id_type=MESH)

    def b_fwd(q, ch, to, kind):
        return pltpu.make_async_remote_copy(
            src_ref=block(q, ch), dst_ref=block(q, ch), send_sem=send.at[kind, ch],
            recv_sem=b_recv.at[q, ch], device_id={"row": to}, device_id_type=MESH)

    def x_back(slot, ch, to):
        return pltpu.make_async_remote_copy(
            src_ref=xst.at[slot], dst_ref=x_ref.at[:, cols(ch)], send_sem=send.at[1, ch],
            recv_sem=x_recv.at[ch], device_id={"row": to}, device_id_type=MESH)

    def l_place(s, j):
        return lbuf.at[s, :, strip_cols(j)]

    def l_own(s, d):
        return pltpu.make_async_remote_copy(
            src_ref=l_ref, dst_ref=l_place(s, col), send_sem=l_send.at[0, d],
            recv_sem=l_recv.at[s, col], device_id={"col": lax.rem(col + d, n_col)}, device_id_type=MESH)

    def l_fwd(s, d):
        return pltpu.make_async_remote_copy(
            src_ref=l_place(s, col), dst_ref=l_place(s, col), send_sem=l_send.at[1, d],
            recv_sem=l_recv.at[s, col], device_id={"col": lax.rem(col + d, n_col)}, device_id_type=MESH)

    def l_cross(s, to, kind):
        return pltpu.make_async_remote_copy(
            src_ref=l_ref, dst_ref=l_place(s, col), send_sem=l_send.at[kind, 0],
            recv_sem=l_recv.at[s, col], device_id={"row": to}, device_id_type=MESH)

    def l_arrival(s, j):
        return pltpu.make_async_remote_copy(
            src_ref=l_ref, dst_ref=l_place(s, j), send_sem=l_send.at[0, 0],
            recv_sem=l_recv.at[s, j], device_id={"col": lax.rem(col + 1, n_col)}, device_id_type=MESH)

    def l_load(s):
        return pltpu.make_async_copy(l_ref, l_place(s, col), l_loc)

    def each(lo, hi, fn):
        def step(i, carry):
            fn(i)
            return carry
        lax.fori_loop(lo, hi, step, 0)

    def dot(s, depth, ch):
        return jnp.dot(lbuf[s, :, :depth], bbuf[ch, :depth, :], preferred_element_type=jnp.float32).astype(xst.dtype)

    def load_start(q, lo, hi):
        each(lo, hi, lambda ch: b_load(q, ch).start())


    def holds(blocks):
        return col < blocks * per_block

    def l_gather_start(s, blocks):
        l_load(s).start()

        @pl.when(holds(blocks))
        def _():
            for d in range(1, n_col):
                l_own(s, d).start()

    def l_gather_wait(s, blocks):
        for j in range(blocks * per_block):
            @pl.when(col != j)
            def _():
                l_arrival(s, j).wait_recv()

    def l_gather_drain(s, blocks):
        @pl.when(holds(blocks))
        def _():
            for d in range(1, n_col):
                l_own(s, d).wait_send()

    def l_relay_start(s, blocks):
        @pl.when(holds(blocks))
        def _():
            l_arrival(s, col).wait_recv()
            for d in range(1, n_col):
                l_fwd(s, d).start()

    def l_relay_drain(s, blocks):
        @pl.when(holds(blocks))
        def _():
            for d in range(1, n_col):
                l_fwd(s, d).wait_send()


    def row0():
        load_start(0, 0, n_ch)
        pl.semaphore_wait(barrier, n_col + 1)
        for i in range(LEAD_A):
            b_own(0, i, 1, 0).start()
        for i in range(LEAD):
            b_own(0, half + i, 3, 1).start()
        each(top, n_ch, lambda ch: b_own(0, ch, 1, 0).start())
        l_gather_start(0, 1)

        def product(ch):
            b_load(0, ch).wait()
            x_ref[:, cols(ch)] = dot(0, m, ch)

        def special(ch):
            product(ch)
            for q in range(1, 4):
                b_fwd(q, ch, 1, 0).wait_recv()
            xst[ch - top] = dot(1, 4 * m, ch)

        def step(k):
            b_own(0, half + k, 1, 0).start()

            @pl.when(k + LEAD_A < half)
            def _():
                b_own(0, k + LEAD_A, 1, 0).start()

            @pl.when(k + LEAD < half)
            def _():
                b_own(0, half + k + LEAD, 3, 1).start()
            b_fwd(1, half + k, 3, 2).wait_recv()
            b_fwd(1, half + k, 3, 2).start()

            @pl.when(k == half - 1)
            def _():
                each(top, n_ch, lambda ch: x_back(ch - top, ch, 3).start())

            @pl.when(k == RELAY)
            def _():
                l_relay_start(1, 4)

            @pl.when(k == LAG)
            def _():
                l_load(0).wait()
                l_gather_wait(0, 1)

            @pl.when(k >= LAG)
            def _():
                done = (k - LAG) * top // (half - LAG)
                each(done, (k + 1 - LAG) * top // (half - LAG), product)

            @pl.when(k == SPECIAL)
            def _():
                l_gather_wait(1, 4)
                each(top, n_ch, special)
        each(0, half, step)

        def drain(k):
            b_own(0, k, 1, 0).wait_send()
            b_own(0, half + k, 1, 0).wait_send()
            b_own(0, half + k, 3, 1).wait_send()
            b_fwd(1, half + k, 3, 2).wait_send()
        each(0, half, drain)

        def drain_special(ch):
            b_own(0, ch, 1, 0).wait_send()
            x_back(ch - top, ch, 3).wait_send()
        each(top, n_ch, drain_special)
        l_gather_drain(0, 1)
        l_relay_drain(1, 4)

    def row1():
        load_start(1, 0, n_ch)
        pl.semaphore_wait(barrier, n_col + 1)
        for i in range(LEAD):
            b_own(1, i, 2, 0).start()
            b_own(1, half + i, 0, 2).start()
        l_gather_start(0, 2)

        def product(ch):
            b_load(1, ch).wait()
            x_ref[:, cols(ch)] = dot(0, 2 * m, ch)

        def late_product(ch):
            b_fwd(0, ch, 2, 1).wait_recv()
            product(ch)

        def special(ch):
            late_product(ch)
            xst[ch - top] = dot(1, 3 * m, ch)

        def special_relay(ch):
            b_own(1, ch, 0, 2).start()
            b_fwd(2, ch, 0, 0).wait_recv()
            b_fwd(2, ch, 0, 0).start()

        def first_done(k):
            return jnp.clip(2 * (k + 1 - LAG), 0, k + 1)

        def second_done(k):
            return jnp.clip(2 * (k + 1 - LAG), 0, jnp.maximum(k + 1 - LEAD_A, 0))

        def step(k):
            b_fwd(0, k, 2, 1).wait_recv()
            b_fwd(0, k, 2, 1).start()

            @pl.when(k + LEAD < half)
            def _():
                b_own(1, k + LEAD, 2, 0).start()
                b_own(1, half + k + LEAD, 0, 2).start()

            @pl.when(k == half - 1)
            def _():
                each(top, n_ch, lambda ch: x_back(ch - top, ch, 2).start())

            @pl.when(k == RELAY)
            def _():
                each(top, n_ch, special_relay)
                l_relay_start(1, 3)

            @pl.when(k == LAG)
            def _():
                l_load(0).wait()
                l_gather_wait(0, 2)
            each(first_done(k - 1), first_done(k), product)
            each(half + second_done(k - 1), half + second_done(k), late_product)

            @pl.when(k == SPECIAL)
            def _():
                l_gather_wait(1, 3)
                each(top, n_ch, special)
        each(0, half, step)
        each(top - LEAD_A, top, late_product)

        def drain(k):
            b_own(1, k, 2, 0).wait_send()
            b_own(1, half + k, 0, 2).wait_send()
            b_fwd(0, k, 2, 1).wait_send()
        each(0, half, drain)

        def drain_special(ch):
            b_own(1, ch, 0, 2).wait_send()
            b_fwd(2, ch, 0, 0).wait_send()
            x_back(ch - top, ch, 2).wait_send()
        each(top, n_ch, drain_special)
        l_gather_drain(0, 2)
        l_relay_drain(1, 3)

    def lower(p):
        o, u = 5 - p, 1 if p == 2 else 0
        s, so = p - 2, o - 2
        base, other = s * half, so * half
        load_start(p, base, base + half)
        pl.semaphore_wait(barrier, n_col + 1)

        @pl.when(holds(p + 1))
        def _():
            l_cross(s, o, 0).start()
            l_cross(1, u, 1).start()
        l_gather_start(s, p + 1)
        each(top, n_ch, lambda ch: b_own(p, ch, u, 0).start())
        each(other, other + half, lambda ch: b_own(p, ch, o, 0).start())
        l_relay_start(so, o + 1)
        l_load(s).wait()
        l_gather_wait(s, p + 1)
        l_gather_wait(so, o + 1)

        def step(ch):
            for q in range(4):
                if q != p:
                    b_fwd(q, ch, o, 0).wait_recv()
            b_load(p, ch).wait()
            away = ch - base
            xst[away] = dot(so, (o + 1) * m, ch)
            x_back(away, ch, o).start()
            x_ref[:, cols(ch)] = dot(s, (p + 1) * m, ch)
        each(base, base + half, step)

        def drain(k):
            b_own(p, other + k, o, 0).wait_send()
            x_back(k, base + k, o).wait_send()
            x_back(k, other + k, o).wait_recv()
        each(0, half, drain)

        def drain_special(ch):
            b_own(p, ch, u, 0).wait_send()
            x_back(ch - top, ch, u).wait_recv()
        each(top, n_ch, drain_special)
        l_gather_drain(s, p + 1)
        l_relay_drain(so, o + 1)

        @pl.when(holds(p + 1))
        def _():
            l_cross(s, o, 0).wait_send()
            l_cross(1, u, 1).wait_send()

    pl.when(row == 0)(row0)
    pl.when(row == 1)(row1)
    pl.when(row == 2)(functools.partial(lower, 2))
    pl.when(row == 3)(functools.partial(lower, 3))


def _store_body(v_ref, x_ref, sem):
    rows = v_ref.shape[0] // STORES
    copies = [pltpu.make_async_copy(v_ref.at[pl.ds(i * rows, rows), :], x_ref.at[pl.ds(i * rows, rows), :], sem.at[i])
              for i in range(STORES)]
    for copy in copies:
        copy.start()
    for copy in copies:
        copy.wait()


def solution(mesh):
    spec = P(("batch", "row"), "col")
    n_row, n_col = mesh.shape["row"], mesh.shape["col"]
    assert n_row == 4

    def local(l_block, b_block):
        m, n = b_block.shape
        k = n_row * m
        n_ch = n // CHUNK
        dma = pltpu.SemaphoreType.DMA
        x = pl.pallas_call(
            functools.partial(_body, n_row, n_col),
            out_shape=pltpu.VMEM((m, n), b_block.dtype),
            in_specs=[pl.BlockSpec(memory_space=pl.ANY)] * 2,
            out_specs=pl.BlockSpec(memory_space=pltpu.VMEM),
            scratch_shapes=[
                pltpu.VMEM((2, m, k), l_block.dtype),
                pltpu.VMEM((n_ch, k, CHUNK), b_block.dtype),
                pltpu.VMEM(((n_ch - DIRECT) // 2, m, CHUNK), b_block.dtype),
                dma((2, n_col)),
                dma((2, n_col)),
                dma(()),
                dma((n_row, n_ch)),
                dma((n_ch,)),
                dma((3, n_ch)),
                dma((n_ch,)),
            ],
            compiler_params=pltpu.CompilerParams(
                collective_id=0, has_side_effects=True, vmem_limit_bytes=50 * 1024 * 1024),
            name="tri_ring",
        )(l_block, b_block)
        return pl.pallas_call(
            _store_body,
            out_shape=jax.ShapeDtypeStruct((m, n), b_block.dtype),
            in_specs=[pl.BlockSpec(memory_space=pltpu.VMEM)],
            out_specs=pl.BlockSpec(memory_space=pl.ANY),
            scratch_shapes=[dma((STORES,))],
            compiler_params=pltpu.CompilerParams(vmem_limit_bytes=1024 * 1024),
            name="tri_store",
        )(pltpu.with_memory_space_constraint(x, pltpu.VMEM))

    return jax.shard_map(local, mesh=mesh, in_specs=(spec, spec), out_specs=spec, check_vma=False)
```

```python
import functools

import jax
import jax.numpy as jnp
from jax import lax
from jax.experimental import pallas as pl
from jax.experimental.pallas import tpu as pltpu
from jax.sharding import PartitionSpec as P

MESH = pl.DeviceIdType.MESH
STEP = 256
STORES = 8


def _pieces(start, widths, index):
    out = []
    for w in widths:
        out.append((start, w, index))
        start, index = start + w, index + 1
    return out


def _body(n_row, n_col, l_ref, b_ref, x_ref, lbuf, bbuf, xst,
          l_recv, l_cross_recv, l_send, l_loc, b_recv, b_loc, send, x_recv, ready, seen, go):
    row = lax.axis_index("row")
    col = lax.axis_index("col")
    m, n = b_ref.shape
    strip = l_ref.shape[1]
    per_block = m // strip
    unit = n // 8
    part = [unit, unit, unit, unit // 2]
    half = sum(part)
    top = 2 * half
    back = unit // 2
    n_back = half // back

    first = _pieces(0, part, 0)
    second = _pieces(half, part, 4)
    second_fine = _pieces(half, part[:3] + [unit // 4] * 2, 4)
    direct = (top, unit, 9)

    barrier = pltpu.get_barrier_semaphore()

    def to_row(sem, r):
        pl.semaphore_signal(sem, inc=1, device_id={"row": r}, device_id_type=MESH)

    def to_peers(sem):
        for d in range(1, n_col):
            pl.semaphore_signal(sem, inc=1, device_id={"col": lax.rem(col + d, n_col)}, device_id_type=MESH)

    def enter_upper(twin, below):
        to_row(barrier, twin)
        to_row(barrier, below)
        to_peers(barrier)
        pl.semaphore_wait(barrier, n_col)

    def await_below():
        pl.semaphore_wait(ready, 1)

    def release_below(twin, below):
        to_row(seen, twin)
        to_peers(seen)
        pl.semaphore_wait(seen, n_col)
        to_row(go, below)

    def enter_lower(above):
        pl.semaphore_wait(barrier, 1)
        to_row(ready, above)

    def all_bytes(ref, sem):
        pltpu.make_async_copy(ref, ref, sem).wait()

    def strip_cols(j):
        return pl.ds(pl.multiple_of(j * strip, strip), strip)

    def block(q, start, w):
        return bbuf.at[pl.ds(q * m, m), pl.ds(start, w)]

    def b_load(q, start, w):
        return pltpu.make_async_copy(b_ref.at[:, pl.ds(start, w)], block(q, start, w), b_loc)

    def b_own(q, piece, to, slot=None):
        start, w, i = piece
        return pltpu.make_async_remote_copy(
            src_ref=b_ref.at[:, pl.ds(start, w)], dst_ref=block(q, start, w), send_sem=send,
            recv_sem=b_recv.at[i if slot is None else slot], device_id={"row": to}, device_id_type=MESH)

    def b_fwd(q, piece, to):
        start, w, i = piece
        return pltpu.make_async_remote_copy(
            src_ref=block(q, start, w), dst_ref=block(q, start, w), send_sem=send,
            recv_sem=b_recv.at[i], device_id={"row": to}, device_id_type=MESH)

    def b_arrive(piece, blocks=1, slot=None):
        start, w, i = piece
        all_bytes(bbuf.at[pl.ds(0, blocks * m), pl.ds(start, w)], b_recv.at[i if slot is None else slot])

    def x_back(base, t, to):
        return pltpu.make_async_remote_copy(
            src_ref=xst.at[:, pl.ds(pl.multiple_of(t * back, back), back)],
            dst_ref=x_ref.at[:, pl.ds(pl.multiple_of(base + t * back, back), back)],
            send_sem=send, recv_sem=x_recv, device_id={"row": to}, device_id_type=MESH)

    def x_direct(to):
        return pltpu.make_async_remote_copy(
            src_ref=xst.at[:, pl.ds(0, unit)], dst_ref=x_ref.at[:, pl.ds(top, unit)],
            send_sem=send, recv_sem=x_recv, device_id={"row": to}, device_id_type=MESH)

    def sent(halves):
        all_bytes(bbuf.at[:, pl.ds(0, halves * unit // 8)], send)

    def l_place(s, j):
        return lbuf.at[s, :, strip_cols(j)]

    def l_own(s, d):
        return pltpu.make_async_remote_copy(
            src_ref=l_ref, dst_ref=l_place(s, col), send_sem=l_send.at[0],
            recv_sem=l_recv.at[s], device_id={"col": lax.rem(col + d, n_col)}, device_id_type=MESH)

    def l_fwd(s, d):
        return pltpu.make_async_remote_copy(
            src_ref=l_place(s, col), dst_ref=l_place(s, col), send_sem=l_send.at[1],
            recv_sem=l_recv.at[s], device_id={"col": lax.rem(col + d, n_col)}, device_id_type=MESH)

    def l_cross(s, to):
        return pltpu.make_async_remote_copy(
            src_ref=l_ref, dst_ref=l_place(s, col), send_sem=l_send.at[0],
            recv_sem=l_cross_recv, device_id={"row": to}, device_id_type=MESH)

    def l_load(s):
        return pltpu.make_async_copy(l_ref, l_place(s, col), l_loc)

    def each(lo, hi, fn):
        def step(i, carry):
            fn(i)
            return carry
        lax.fori_loop(lo, hi, step, 0)

    def multiply(s, depth, out, shift, start, w):
        def step(i):
            c = pl.multiple_of(start + i * STEP, STEP)
            product = jnp.dot(lbuf[s, :, :depth], bbuf[:depth, pl.ds(c, STEP)], preferred_element_type=jnp.float32)
            out[:, pl.ds(pl.multiple_of(c - shift, STEP), STEP)] = product.astype(out.dtype)
        each(0, w // STEP, step)


    def holds(blocks):
        return col < blocks * per_block

    def l_gather_start(s, blocks):
        l_load(s).start()

        @pl.when(holds(blocks))
        def _():
            for d in range(1, n_col):
                l_own(s, d).start()

    def l_gather_wait(s, blocks):
        count = blocks * per_block

        @pl.when(holds(blocks))
        def _():
            all_bytes(lbuf.at[s, :, pl.ds(0, (count - 1) * strip)], l_recv.at[s])

        @pl.when(jnp.logical_not(holds(blocks)))
        def _():
            all_bytes(lbuf.at[s, :, pl.ds(0, count * strip)], l_recv.at[s])

    def l_gather_drain(blocks, crossed):
        @pl.when(holds(blocks))
        def _():
            all_bytes(lbuf.at[:, :, pl.ds(0, (n_col - 1 + crossed) * strip // 2)], l_send.at[0])

    def l_relay_start(s, blocks):
        @pl.when(holds(blocks))
        def _():
            all_bytes(l_place(s, col), l_cross_recv)
            for d in range(1, n_col):
                l_fwd(s, d).start()

    def l_relay_drain(blocks):
        @pl.when(holds(blocks))
        def _():
            all_bytes(lbuf.at[0, :, pl.ds(0, (n_col - 1) * strip)], l_send.at[1])

    def row0():
        enter_upper(1, 3)
        for piece in first[:2] + [direct] + first[2:] + second_fine:
            b_own(0, piece, 1).start()
        await_below()
        for piece in second[:2]:
            b_own(0, piece, 3).start()
        b_load(0, 0, n).start()
        release_below(1, 3)
        l_gather_start(0, 1)
        for piece in second[:2]:
            b_arrive(piece)
            b_fwd(1, piece, 3).start()
        b_own(0, second[2], 3).start()
        l_relay_start(1, 4)
        l_load(0).wait()
        l_gather_wait(0, 1)
        b_load(0, 0, n).wait()
        multiply(0, m, x_ref, 0, 0, half)
        b_arrive(second[2])
        b_fwd(1, second[2], 3).start()
        b_own(0, second[3], 3).start()
        b_arrive(second[3])
        b_fwd(1, second[3], 3).start()
        multiply(0, m, x_ref, 0, half, n - half)
        l_gather_wait(1, 4)
        b_arrive(direct, 3)
        multiply(1, 4 * m, xst, top, top, unit)
        x_direct(3).start()
        l_gather_drain(1, 0)
        l_relay_drain(4)
        sent(32)

    def row1():
        enter_upper(0, 2)
        for piece in second + [direct]:
            b_own(1, piece, 0).start()
        await_below()
        for piece in first[:2]:
            b_own(1, piece, 2).start()
        b_load(1, 0, n).start()
        release_below(0, 2)
        l_gather_start(0, 2)

        def pass_on(piece):
            b_arrive(piece)
            b_fwd(0, piece, 2).start()

        pass_on(first[0])
        b_arrive(direct, slot=10)
        b_fwd(2, direct, 0).start()
        l_relay_start(1, 3)
        pass_on(first[1])
        b_own(1, first[2], 2).start()
        l_load(0).wait()
        l_gather_wait(0, 2)
        b_load(1, 0, n).wait()
        multiply(0, 2 * m, x_ref, 0, 0, 2 * unit)
        b_arrive(direct)
        l_gather_wait(1, 3)
        multiply(1, 3 * m, xst, top, top, unit)
        pass_on(first[2])
        b_own(1, first[3], 2).start()
        pass_on(first[3])
        x_direct(2).start()
        multiply(0, 2 * m, x_ref, 0, 2 * unit, half - 2 * unit)
        multiply(0, 2 * m, x_ref, 0, top, unit)
        l_gather_drain(2, 0)
        l_relay_drain(3)
        for piece in second_fine:
            b_arrive(piece)
            multiply(0, 2 * m, x_ref, 0, piece[0], piece[1])
        sent(27)

    def lower(p):
        o, u = 5 - p, 1 if p == 2 else 0
        s, so = p - 2, o - 2
        mine, others = (first, second) if p == 2 else (second, first)
        base = mine[0][0]
        enter_lower(u)
        b_load(p, base, half).start()

        @pl.when(holds(p + 1))
        def _():
            l_cross(1, u).start()
        b_own(p, direct, u, 10 if p == 2 else None).start()
        pl.semaphore_wait(go, 1)

        @pl.when(holds(p + 1))
        def _():
            l_cross(s, o).start()
        l_gather_start(s, p + 1)
        for piece in others:
            b_own(p, piece, o).start()
        l_relay_start(so, o + 1)
        l_load(s).wait()
        l_gather_wait(s, p + 1)
        l_gather_wait(so, o + 1)
        l_gather_drain(p + 1, 2)
        l_relay_drain(o + 1)
        b_load(p, base, half).wait()

        for piece in mine:
            b_arrive(piece, 3)
            start, w, _ = piece

            def away(t):
                multiply(so, (o + 1) * m, xst, base, base + t * back, back)
                x_back(base, t, o).start()
            each((start - base) // back, (start - base + w) // back, away)
            multiply(s, (p + 1) * m, x_ref, 0, start, w)

        sent(16)
        all_bytes(x_ref.at[:, pl.ds(0, half + unit)], x_recv)

    pl.when(row == 0)(row0)
    pl.when(row == 1)(row1)
    pl.when(row == 2)(functools.partial(lower, 2))
    pl.when(row == 3)(functools.partial(lower, 3))


def _store_body(v_ref, x_ref, sem):
    rows = v_ref.shape[0] // STORES
    copies = [pltpu.make_async_copy(v_ref.at[pl.ds(i * rows, rows), :], x_ref.at[pl.ds(i * rows, rows), :], sem.at[i])
              for i in range(STORES)]
    for copy in copies:
        copy.start()
    for copy in copies:
        copy.wait()


def solution(mesh):
    spec = P(("batch", "row"), "col")
    n_row, n_col = mesh.shape["row"], mesh.shape["col"]
    assert n_row == 4

    def local(l_block, b_block):
        m, n = b_block.shape
        k = n_row * m
        half = 7 * n // 16
        dma = pltpu.SemaphoreType.DMA
        x = pl.pallas_call(
            functools.partial(_body, n_row, n_col),
            out_shape=pltpu.VMEM((m, n), b_block.dtype),
            in_specs=[pl.BlockSpec(memory_space=pl.ANY)] * 2,
            out_specs=pl.BlockSpec(memory_space=pltpu.VMEM),
            scratch_shapes=[
                pltpu.VMEM((2, m, k), l_block.dtype),
                pltpu.VMEM((k, n), b_block.dtype),
                pltpu.VMEM((m, half), b_block.dtype),
                dma((2,)),
                dma(()),
                dma((2,)),
                dma(()),
                dma((11,)),
                dma(()),
                dma(()),
                dma(()),
                pltpu.SemaphoreType.REGULAR,
                pltpu.SemaphoreType.REGULAR,
                pltpu.SemaphoreType.REGULAR,
            ],
            compiler_params=pltpu.CompilerParams(
                collective_id=0, has_side_effects=True, vmem_limit_bytes=50 * 1024 * 1024),
            name="tri_ring",
        )(l_block, b_block)
        return pl.pallas_call(
            _store_body,
            out_shape=jax.ShapeDtypeStruct((m, n), b_block.dtype),
            in_specs=[pl.BlockSpec(memory_space=pltpu.VMEM)],
            out_specs=pl.BlockSpec(memory_space=pl.ANY),
            scratch_shapes=[dma((STORES,))],
            compiler_params=pltpu.CompilerParams(vmem_limit_bytes=1024 * 1024),
            name="tri_store",
        )(pltpu.with_memory_space_constraint(x, pltpu.VMEM))

    return jax.shard_map(local, mesh=mesh, in_specs=(spec, spec), out_specs=spec, check_vma=False)
```
